32 devices in a mesh: row: 8 (over y, x, core), col: 4 (over z).
Axes of the slice: x: 2, y: 2, z: 4, core: 2. Of those that a mesh axis runs over, the one named last changes fastest.
Arguments:
- vectors: float32 [16384, 16384], P('row', 'col'), may hold values from -0.046875 to 0.046875
- basis: float32 [16384, 2048], P('col', 'row'), may hold values from -9 to 9
- block_units: int32 [8], replicated, may hold values from 1 to 40, 64 in all
Outputs:
- assembled: float32 [16384, 2048], P('row', 'col')
The draws below stay inside these ranges and needn't reach their ends.
Inputs may be any that keep to these rules, and one draw needn't show every extreme that they name: `block_units`: the block sizes are whole numbers of units that sum to 64; the largest is exactly the maximum.
All inputs are finite; a program needn't handle non-finite values.
Results may differ from the reference program's by a relative error of at most 0.00007.
Values sent between devices are 32-bit elements; how exact they have to be, the bound alone decides.
A program may use at most 192 MiB of HBM per device.

```python
import math
import jax
import jax.numpy as jnp
import numpy as np
from jax import lax

N = 16384
W = 2048
UNIT = 256
BLOCKS = 8
START = 7168


def block_scale(own_key, extent, cuts, smallest, largest):
    def one(axis_at, shards_of):
        heights = jax.random.uniform(jax.random.fold_in(jax.random.fold_in(own_key, 6), axis_at), (shards_of,), jnp.float32, smallest / len(cuts), largest / len(cuts))
        return jnp.repeat(jnp.exp(heights), extent[axis_at] // shards_of).reshape((-1,) + (1,) * (len(extent) - axis_at - 1))

    level = one(*cuts[0])
    for cut in cuts[1:]:
        level = level * one(*cut)
    return level


def length_profile(count, total, reach, skew):
    weights = [(1 << 20) // math.isqrt(standing ** skew) + 1 for standing in range(2, count + 1)]
    surplus, counts = total - reach - (count - 1), [1] * (count - 1)
    while surplus > 0:
        candidates = [i for i in range(count - 1) if counts[i] < reach]
        mass, left = sum([weights[i] for i in candidates]), surplus
        for i in candidates:
            extra = min(reach - counts[i], max(1, left * weights[i] // mass), surplus)
            counts[i] = counts[i] + extra
            surplus = surplus - extra
    return np.array([reach] + counts)


def uneven_parts(key, amount, total, most, slope):
    if amount == 2:
        one = jax.random.randint(key, (), max(1, total - most), min(most, total - 1) + 1)
        return jnp.stack([one, total - one])
    tallies = jnp.asarray(length_profile(amount, total, most, slope), jnp.int32)
    couples = (amount - 1) // 2
    donor, receiver = tallies[1:1 + 2 * couples:2], tallies[2:2 + 2 * couples:2]
    room = jnp.minimum(donor - 1, most - receiver)
    moved = jax.random.randint(jax.random.fold_in(key, 1), (couples,), 0, 1 << 20) % (room + 1)
    tallies = tallies.at[1:1 + 2 * couples:2].set(donor - moved).at[2:2 + 2 * couples:2].set(receiver + moved)
    return tallies[jax.random.permutation(jax.random.fold_in(key, 2), amount)]


def bell_draw(own_key, dims, spread, bound, pieces=(), held_as=jnp.bfloat16):
    array = spread * jax.random.normal(own_key, dims, jnp.float32)
    if pieces:
        array = array * block_scale(own_key, dims, pieces, -0.22, 0.18)
    return jnp.clip(array, -bound, bound).astype(held_as)


def setup_inputs(seed: int = 0) -> dict:
    key_list = jax.random.split(jax.random.key(seed), 4)
    return {
        "vectors": bell_draw(key_list[0], (N, N), N ** -0.5, 0.046875, ((0, 8), (1, 4)), jnp.float32),
        "basis": bell_draw(key_list[1], (N, W), 1.5, 9.0, ((0, 4), (1, 8)), jnp.float32),
        "block_units": uneven_parts(key_list[2], BLOCKS, N // UNIT, 5 * N // (8 * UNIT), 2).astype(jnp.int32),
    }


def block_ids(positions, block_units):
    ends = jnp.cumsum(block_units).astype(jnp.int32) * UNIT
    return jnp.sum((positions[:, None] >= ends[None, :-1]).astype(jnp.int32), axis=1)


def reference(vectors, basis, block_units):
    row_block = block_ids(jnp.arange(N, dtype=jnp.int32), block_units)
    slab_block = block_ids(START + jnp.arange(W, dtype=jnp.int32), block_units)
    masked = jnp.where(row_block[:, None] == slab_block[None, :], basis, jnp.float32(0.0))
    return jnp.dot(vectors, masked, precision=lax.Precision.HIGHEST, preferred_element_type=jnp.float32)
```

```python
import functools

import jax
import jax.numpy as jnp
from jax import lax
from jax.experimental import pallas as pl
from jax.experimental.pallas import tpu as pltpu
from jax.sharding import PartitionSpec as P

UNIT = 256
START = 7168
LANES = 128
PIECE = 512
STAGE = 64
LAG = 4
VMEM_BYTES = 67043328
MESH = pl.DeviceIdType.MESH


def block_ids(positions, block_units):
    ends = jnp.cumsum(block_units) * UNIT
    return jnp.sum((positions[:, None] >= ends[None, :-1]).astype(jnp.int32), axis=1)


def plain(vectors, basis, block_units):
    inner, width = basis.shape
    row_block = block_ids(
        lax.axis_index("col") * inner + jnp.arange(inner, dtype=jnp.int32), block_units
    )
    slab_block = block_ids(
        START + lax.axis_index("row") * width + jnp.arange(width, dtype=jnp.int32), block_units
    )
    masked = jnp.where(row_block[:, None] == slab_block[None, :], basis, jnp.float32(0.0))

    rows, cols = lax.axis_size("row"), lax.axis_size("col")
    step = LANES if width % LANES == 0 and rows % cols == 0 else width
    pieces = [
        lax.all_gather(masked[:, at:at + step], "row", axis=1, tiled=True)
        for at in range(0, width, step)
    ]
    sums = []
    for piece in pieces:
        part = jnp.dot(
            vectors, piece, precision=lax.Precision.HIGH, preferred_element_type=jnp.float32
        )
        sums.append(lax.psum_scatter(part, "col", scatter_dimension=1, tiled=True))
    groups = sums[0].shape[1] // step
    return jnp.concatenate(
        [one[:, g * step:(g + 1) * step] for g in range(groups) for one in sums], axis=1
    )


def pick(at, values):
    out = values[-1]
    for i in range(len(values) - 2, -1, -1):
        out = jnp.where(at == i, values[i], out)
    return out


def kernel(rows, cols, blocks, units_ref, v_ref, b_ref, out_ref, gath, in_r, in_l,
           vh, vl, part, vst, mst, mh, ml, held,
           v_sem, m_sem, h_sem, o_sem, link_send, link_recv, twin_send, twin_recv,
           z_send, right_recv, left_recv):
    row, c = lax.axis_index("row"), lax.axis_index("col")
    last = cols - 1
    core = row % 2
    chip = row // 2
    x, y = chip % 2, chip // 2
    chip_x = y * 2 + (1 - x)
    chip_y = (1 - y) * 2 + x
    chip_d = (1 - y) * 2 + (1 - x)
    twin = chip * 2 + (1 - core)
    mrows, inner = v_ref.shape
    per_block = 2 * rows // cols
    pieces = mrows // PIECE
    chunks = rows
    slots = (cols - 1) * per_block

    peer = [
        None,
        jnp.where(core == 0, chip_x, chip_y) * 2 + core,
        jnp.where(core == 0, chip_y, chip_x) * 2 + core,
        jnp.where(core == 0, chip_x, chip_y) * 2 + core,
    ]

    def unit_a(q):
        ph, h = q // 2, q % 2
        return 2 * pick(ph, [row, chip_x * 2, chip_x * 2 + 1, chip_d * 2 + core]) + h

    def unit_b(q):
        ph, h = q // 2, q % 2
        return 2 * pick(ph, [twin, chip_y * 2 + 1, chip_y * 2, chip_d * 2 + (1 - core)]) + h

    def unit_mine(q):
        ph, h = q // 2, q % 2
        return 2 * pick(ph, [row, peer[1], peer[2], chip_d * 2 + (1 - core)]) + h

    def own_cols(h):
        return b_ref.at[:, pl.ds(pl.multiple_of(h * LANES, LANES), LANES)]

    def link_copy(ph, h):
        q = 2 * ph + h
        u = 2 * row + h
        if ph == 3:
            u = 2 * jnp.where(core == 0, chip_y * 2 + 1, chip_x * 2) + h
        return pltpu.make_async_remote_copy(
            src_ref=gath.at[u] if ph == 3 else own_cols(h), dst_ref=gath.at[u],
            send_sem=link_send.at[q], recv_sem=link_recv.at[q],
            device_id=(peer[ph], c), device_id_type=MESH)

    def link_arrival(q):
        u = unit_mine(q)
        return pltpu.make_async_remote_copy(
            src_ref=gath.at[u], dst_ref=gath.at[u],
            send_sem=link_send.at[q], recv_sem=link_recv.at[q],
            device_id=(twin, c), device_id_type=MESH)

    def twin_own(h):
        return pltpu.make_async_remote_copy(
            src_ref=own_cols(h), dst_ref=gath.at[2 * row + h],
            send_sem=twin_send.at[h], recv_sem=twin_recv.at[h],
            device_id=(twin, c), device_id_type=MESH)

    def twin_copy(q):
        u = unit_mine(q)
        return pltpu.make_async_remote_copy(
            src_ref=gath.at[u], dst_ref=gath.at[u],
            send_sem=twin_send.at[q], recv_sem=twin_recv.at[q],
            device_id=(twin, c), device_id_type=MESH)

    def z_copy(u, s, right):
        at = pl.ds(pl.multiple_of(s * PIECE, PIECE), PIECE)
        return pltpu.make_async_remote_copy(
            src_ref=part.at[u, at], dst_ref=(in_r if right else in_l).at[u, at],
            send_sem=z_send.at[u, s],
            recv_sem=(right_recv if right else left_recv).at[u, s],
            device_id=(row, c + 1 if right else c - 1), device_id_type=MESH)

    barrier = pltpu.get_barrier_semaphore()
    near = [twin, peer[1], peer[2]]
    for other in near:
        pl.semaphore_signal(barrier, inc=1, device_id=(other, c), device_id_type=MESH)

    @pl.when(c > 0)
    def _():
        pl.semaphore_signal(barrier, inc=1, device_id=(row, c - 1), device_id_type=MESH)

    @pl.when(c < last)
    def _():
        pl.semaphore_signal(barrier, inc=1, device_id=(row, c + 1), device_id_type=MESH)

    def v_copy(i, slot):
        return pltpu.make_async_copy(
            v_ref.at[pl.ds(pl.multiple_of(i * STAGE, STAGE), STAGE)], vst.at[slot], v_sem.at[slot])

    v_copy(0, 0).start()
    v_copy(1, 1).start()
    line = jnp.where(c > 0, 1, 0) + jnp.where(c < last, 1, 0)
    pl.semaphore_wait(barrier, len(near) + line)

    for h in range(2):
        twin_own(h).start()
    for h in range(2):
        link_copy(1, h).start()

    v_steps = mrows // STAGE

    def v_body(i, _):
        slot = i % 2
        v_copy(i, slot).wait()
        at = pl.ds(pl.multiple_of(i * STAGE, STAGE), STAGE)
        val = vst[slot]
        hi = val.astype(jnp.bfloat16)
        vh[at, :] = hi
        vl[at, :] = (val - hi.astype(jnp.float32)).astype(jnp.bfloat16)

        @pl.when(i + 2 < v_steps)
        def _():
            v_copy(i + 2, slot).start()
        return 0

    lax.fori_loop(0, v_steps, v_body, 0)

    ends, total = [], jnp.int32(0)
    for i in range(blocks - 1):
        total = total + units_ref[i]
        ends.append(total * UNIT)

    def block_of(position):
        got = jnp.int32(0)
        for end in ends:
            got = got + jnp.where(position >= end, 1, 0)
        return got

    def m_copy(src, slot):
        return pltpu.make_async_copy(src, mst.at[slot], m_sem.at[slot])

    def slot_unit(t, skipped):
        mixed = 4 + 2 * (t - 4) + jnp.where(skipped == chip_x, 1, 0)
        mixed = jnp.where(t < 4, t, jnp.where(t < 8, mixed, t + 4))
        n = jnp.where(skipped == chip, t + 4, jnp.where(skipped == chip_d, t, mixed))
        q = n // 2
        return jnp.where(n % 2 == 0, unit_a(q), unit_b(q))

    def forward(u, s, right):
        z_copy(u, s, right).wait_recv()
        at = pl.ds(pl.multiple_of(s * PIECE, PIECE), PIECE)
        local = pltpu.make_async_copy((in_r if right else in_l).at[u, at], held, h_sem)
        local.start()
        local.wait()
        part[u, at, :] = part[u, at, :] + held[...]
        z_copy(u, s, right).start()

    steps = slots * pieces
    right_lag, left_lag = (c - 1) * LAG, (last - 1 - c) * LAG

    def handle(first, count):
        def body(at, _):
            r, l = at - right_lag, at - left_lag
            rt, lt = jnp.maximum(r, 0) // pieces, jnp.maximum(l, 0) // pieces
            ur = slot_unit(jnp.minimum(rt, slots - 1), 0)
            ul = slot_unit(jnp.minimum(lt, slots - 1), last)

            @pl.when((c > 0) & (c < ur // per_block) & (r >= 0) & (r < steps))
            def _():
                forward(ur, r % pieces, True)

            @pl.when((c < last) & (c > ul // per_block) & (l >= 0) & (l < steps))
            def _():
                forward(ul, l % pieces, False)
            return 0

        lax.fori_loop(first, first + count, body, 0)

    early = jnp.where(chip == c, 1, 0)

    def next_chunk(at):
        return (at + 2 * early) % chunks

    def chunk(at_chunk, _):
        q, following = next_chunk(at_chunk), next_chunk(at_chunk + 1)
        ua, ub = unit_a(q), unit_b(q)
        h = q % 2
        twin_wait = pltpu.make_async_remote_copy(
            src_ref=gath.at[ub], dst_ref=gath.at[ub], send_sem=twin_send.at[q],
            recv_sem=twin_recv.at[q], device_id=(twin, c), device_id_type=MESH)
        twin_wait.wait_recv()

        @pl.when(q == 3)
        def _():
            for hh in range(2):
                link_copy(3, hh).start()

        @pl.when(q < 2)
        def _():
            m_copy(own_cols(h), 0).start()

        @pl.when(q >= 2)
        def _():
            m_copy(gath.at[ua], 0).start()

        m_copy(gath.at[ub], 1).start()
        m_copy(gath.at[ub], 0).wait()
        m_copy(gath.at[ub], 1).wait()

        sa, sb = block_of(START + ua * LANES), block_of(START + ub * LANES)

        def split(g, _):
            at = pl.ds(pl.multiple_of(g * UNIT, UNIT), UNIT)
            mine = block_of(c * inner + g * UNIT)
            for a, sl in ((0, sa), (1, sb)):
                keep = jnp.where(mine == sl, jnp.float32(1.0), jnp.float32(0.0))
                val = mst[a, at, :] * keep
                hi = val.astype(jnp.bfloat16)
                mh[at, a * LANES:(a + 1) * LANES] = hi
                ml[at, a * LANES:(a + 1) * LANES] = (val - hi.astype(jnp.float32)).astype(jnp.bfloat16)
            return 0

        lax.fori_loop(0, inner // UNIT, split, 0)

        def multiply(s, _):
            at = pl.ds(pl.multiple_of(s * PIECE, PIECE), PIECE)
            acc = jnp.dot(vl[at, :], mh[...], preferred_element_type=jnp.float32)
            acc = jnp.dot(vh[at, :], ml[...], preferred_element_type=jnp.float32) + acc
            acc = jnp.dot(vh[at, :], mh[...], preferred_element_type=jnp.float32) + acc
            part[ua, at, :] = acc[:, :LANES]
            part[ub, at, :] = acc[:, LANES:]
            for u in (ua, ub):
                @pl.when((c == 0) & (u // per_block > 0))
                def _():
                    z_copy(u, s, True).start()

                @pl.when((c == last) & (u // per_block < last))
                def _():
                    z_copy(u, s, False).start()
            return 0

        lax.fori_loop(0, pieces, multiply, 0)

        @pl.when((following >= 2) & (at_chunk < chunks - 1))
        def _():
            link_arrival(following).wait_recv()
            twin_copy(following).start()

        @pl.when(at_chunk == 1 - early)
        def _():
            for hh in range(2):
                link_copy(2, hh).start()

        @pl.when(at_chunk >= 2)
        def _():
            handle((at_chunk - 2) * 2 * pieces, 2 * pieces)
        return 0

    @pl.when(chip == c)
    def _():
        link_arrival(2).wait_recv()
        twin_copy(2).start()

    lax.fori_loop(0, chunks, chunk, 0)
    handle(steps, LAG * (cols - 2))

    def landed(u, right):
        return pltpu.make_async_copy(
            (in_r if right else in_l).at[u], mst.at[0 if right else 1, pl.ds(0, mrows)],
            m_sem.at[0 if right else 1])

    def finish(i, _):
        u = c * per_block + i
        sides = ((True, c > 0), (False, c < last))
        for right, there in sides:
            @pl.when(there)
            def _():
                for s in range(pieces):
                    z_copy(u, s, right).wait_recv()
                landed(u, right).start()
        for right, there in sides:
            @pl.when(there)
            def _():
                landed(u, right).wait()

                def add(s, _):
                    at = pl.ds(pl.multiple_of(s * PIECE, PIECE), PIECE)
                    part[u, at, :] = part[u, at, :] + mst[0 if right else 1, at, :]
                    return 0

                lax.fori_loop(0, pieces, add, 0)
        out_copy(i).start()
        return 0

    def out_copy(i):
        return pltpu.make_async_copy(
            part.at[c * per_block + i],
            out_ref.at[:, pl.ds(pl.multiple_of(i * LANES, LANES), LANES)], o_sem.at[i])

    lax.fori_loop(0, per_block, finish, 0)

    for h in range(2):
        twin_own(h).wait_send()
    for q in range(2, chunks):
        twin_copy(q).wait_send()
        link_copy(q // 2, q % 2).wait_send()

    def drain(u, _):
        @pl.when(u // per_block != c)
        def _():
            for s in range(pieces):
                z_copy(u, s, True).wait_send()
        return 0

    lax.fori_loop(0, 2 * rows, drain, 0)
    for i in range(per_block):
        out_copy(i).wait()


def fused(rows, cols, vectors, basis, block_units):
    mrows, inner = vectors.shape
    units = 2 * rows
    pieces = mrows // PIECE
    f32, bf16 = jnp.float32, jnp.bfloat16
    any_space = pl.BlockSpec(memory_space=pl.ANY)
    dma = pltpu.SemaphoreType.DMA
    flops = 6 * mrows * inner * units * LANES
    return pl.pallas_call(
        functools.partial(kernel, rows, cols, block_units.shape[0]),
        out_shape=[
            jax.ShapeDtypeStruct((mrows, units * LANES // cols), f32),
            jax.ShapeDtypeStruct((units, inner, LANES), f32),
            jax.ShapeDtypeStruct((units, mrows, LANES), f32),
            jax.ShapeDtypeStruct((units, mrows, LANES), f32),
        ],
        in_specs=[pl.BlockSpec(memory_space=pltpu.SMEM), any_space, any_space],
        out_specs=[any_space] * 4,
        scratch_shapes=[
            pltpu.VMEM((mrows, inner), bf16),
            pltpu.VMEM((mrows, inner), bf16),
            pltpu.VMEM((units, mrows, LANES), f32),
            pltpu.VMEM((2, STAGE, inner), f32),
            pltpu.VMEM((2, inner, LANES), f32),
            pltpu.VMEM((inner, 2 * LANES), bf16),
            pltpu.VMEM((inner, 2 * LANES), bf16),
            pltpu.VMEM((PIECE, LANES), f32),
            dma((2,)), dma((2,)), dma, dma((units // cols,)),
            dma((rows,)), dma((rows,)), dma((rows,)), dma((rows,)),
            dma((units, pieces)), dma((units, pieces)), dma((units, pieces)),
        ],
        compiler_params=pltpu.CompilerParams(
            collective_id=0, has_side_effects=True, vmem_limit_bytes=VMEM_BYTES),
        cost_estimate=pl.CostEstimate(flops=flops, bytes_accessed=4 * mrows * inner, transcendentals=0),
    )(block_units, vectors, basis)[0]


def solution(mesh):
    rows, cols = mesh.shape["row"], mesh.shape["col"]

    def shards(vectors, basis, block_units):
        fits = rows // 2 == cols == 4 and basis.shape[1] == 2 * LANES
        if fits and vectors.shape[0] % PIECE == 0 and vectors.shape[1] % UNIT == 0:
            return fused(rows, cols, vectors, basis, block_units)
        return plain(vectors, basis, block_units)

    in_specs = (P("row", "col"), P("col", "row"), P())
    return jax.shard_map(
        shards, mesh=mesh, in_specs=in_specs, out_specs=P("row", "col"), check_vma=False)
```
